32 devices in a mesh: groups: 2 (over y), seq: 4 (over z), heads: 2 (over x), cfg: 2 (over core).
Axes of the slice: x: 2, y: 2, z: 4, core: 2. Of those that a mesh axis runs over, the one named last changes fastest.
Arguments:
- video_tokens: bfloat16 [2, 8, 1152, 1024], P('cfg', ('groups', 'seq'), 'heads'), parts along dimension 1, may hold values from -6 to 6
- text_tokens: bfloat16 [2, 8, 1152, 128], P('cfg', ('groups', 'seq'), 'heads'), parts along dimension 1, may hold values from -6 to 6
- text_length: int32 [2, 8], P('cfg', ('groups', 'seq')), parts along dimension 1, may hold values from 1 to 128
- guide_numer: int32 [8], P(('groups', 'seq')), parts along dimension 0, may hold values from 2 to 8
- guide_denom: int32 [8], P(('groups', 'seq')), parts along dimension 0, may hold values from 4 to 8
- spatial_gain: bfloat16 [1152], replicated, may hold values from 0.25 to 1.75
- spatial_qkv: bfloat16 [3, 1152, 1152], P(None, 'heads'), may hold values from -0.11785113 to 0.11785113
- spatial_out: bfloat16 [1152, 1152], P('heads'), may hold values from -0.1875 to 0.1875
- temporal_gain: bfloat16 [1152], replicated, may hold values from 0.25 to 1.75
- temporal_qkv: bfloat16 [3, 1152, 1152], P(None, 'heads'), may hold values from -0.11785113 to 0.11785113
- temporal_out: bfloat16 [1152, 1152], P('heads'), may hold values from -0.1875 to 0.1875
Outputs:
- guided: bfloat16 [8, 1152, 1024], P(('groups', 'seq'), ('heads', 'cfg')), parts along dimension 0
The draws below stay inside these ranges and needn't reach their ends.
There are 2 independent parts, one for each index of `groups`. The reference program is written for one: setup_inputs(seed, part) draws one part's arguments, and reference() takes and returns one part's arrays. A program takes and returns all parts, laid end to end along the dimension named above; an argument that names none is the same for every part. Nothing has to cross between parts.
Inputs may be any that keep to these rules, and one draw needn't show every extreme that they name: `text_length`: text tokens at or beyond a frame's length are padding.
All inputs are finite; a program needn't handle non-finite values.
Results may differ from the reference program's by a relative error of at most 0.009.
Values may be sent and summed in bfloat16 or wider, within the bound.
A program may use at most 64 MiB of HBM per device.

```python
import jax
import jax.numpy as jnp
from jax import lax

D = 1152
HEADS = 16
HEAD_DIM = 72
POS = 1024
TXT = 128
FRAMES = 4


def projection_law(key):
    sigma = D ** (-0.5)
    first = jax.random.fold_in(key, 0)
    values = jnp.clip(jax.random.normal(first, (3, D, D), jnp.float32), -4.0, 4.0) * sigma
    return values.astype(jnp.bfloat16)


def draw_spatial_qkv(key, part):
    return projection_law(jax.random.fold_in(key, 11))


def draw_temporal_qkv(key, part):
    return projection_law(jax.random.fold_in(key, 23))


def draw_video_tokens(key, part):
    key = jax.random.fold_in(key, 31)
    first = jax.random.fold_in(key, 0)
    shape = (2, FRAMES, D, POS)
    values = jnp.clip(jax.random.normal(first, shape, jnp.float32), -6.0, 6.0)
    return values.astype(jnp.bfloat16)


def touch_ends(entries, own_key, low, top_value):
    longest = entries.shape.index(max(entries.shape))
    spots = []
    for shift in (0, 1):
        where = [jax.random.randint(jax.random.fold_in(own_key, axis), (), 0, length) for axis, length in enumerate(entries.shape)]
        where[longest] = (where[longest] + shift) % entries.shape[longest]
        spots.append(tuple(where))
    return entries.at[spots[0]].set(low).at[spots[1]].set(top_value)


def level_of(stream_key, shape, cuts, least, largest):
    level, own = 1.0, jax.random.fold_in(stream_key, 6)
    for position, shards_of in cuts:
        steps = jnp.exp(jax.random.uniform(jax.random.fold_in(own, position), (shards_of,), jnp.float32, least / len(cuts), largest / len(cuts)))
        level = level * jnp.repeat(steps, shape[position] // shards_of).reshape([-1 if axis == position else 1 for axis in range(len(shape))])
    return level


def normal_values(stream_key, shape, scale, most, pieces=(), kind=jnp.bfloat16):
    drawn = jax.random.normal(stream_key, shape, jnp.float32) * scale
    if len(pieces) > 0:
        drawn = level_of(stream_key, shape, pieces, -0.22, 0.18) * drawn
    return jnp.clip(drawn, min=-most, max=most).astype(kind)


def setup_inputs(seed: int = 0, part: int = 0) -> dict:
    key_list = jax.random.split(jax.random.key(seed), 12)
    own_keys = jax.random.split(jax.random.fold_in(key_list[11], part), 12)
    video_tokens = draw_video_tokens(jax.random.fold_in(jax.random.fold_in(key_list[11], part), 71), part)
    text_tokens = normal_values(own_keys[1], (2, FRAMES, D, TXT), 1.0, 6.0, ((0, 2), (1, 4), (2, 2)))
    text_length = touch_ends(jax.random.randint(own_keys[2], (2, FRAMES), 1, TXT + 1), jax.random.fold_in(own_keys[2], 1), 1, TXT).astype(jnp.int32)
    guide_numer = touch_ends(jax.random.randint(own_keys[3], (FRAMES,), 2, 9), jax.random.fold_in(own_keys[3], 1), 2, 8).astype(jnp.int32)
    guide_denom = touch_ends(jax.random.randint(own_keys[4], (FRAMES,), 4, 9), jax.random.fold_in(own_keys[4], 1), 4, 8).astype(jnp.int32)
    spatial_gain = jnp.clip(1.0 + 0.15 * jax.random.normal(key_list[5], (D,), jnp.float32), 0.25, 1.75).astype(jnp.bfloat16)
    spatial_qkv = draw_spatial_qkv(jax.random.fold_in(key_list[11], 71), part)
    spatial_out = normal_values(key_list[7], (D, D), D ** -0.5, 0.1875, ((0, 2),))
    temporal_gain = jnp.clip(1.0 + 0.15 * jax.random.normal(key_list[8], (D,), jnp.float32), 0.25, 1.75).astype(jnp.bfloat16)
    temporal_qkv = draw_temporal_qkv(jax.random.fold_in(key_list[11], 71), part)
    temporal_out = normal_values(key_list[10], (D, D), D ** -0.5, 0.1875, ((0, 2),))
    return dict(video_tokens=video_tokens, text_tokens=text_tokens, text_length=text_length, guide_numer=guide_numer, guide_denom=guide_denom, spatial_gain=spatial_gain, spatial_qkv=spatial_qkv, spatial_out=spatial_out, temporal_gain=temporal_gain, temporal_qkv=temporal_qkv, temporal_out=temporal_out)


epsilon = 1e-06

def normed_project(token_rows, gain_vector, weight_matrix):
    values_wide = token_rows.astype(jnp.float32)
    inverse = lax.rsqrt(lax.optimization_barrier(jnp.mean(values_wide * values_wide, axis=-1)) + epsilon)
    scaled = (values_wide * gain_vector.astype(jnp.float32)).astype(jnp.bfloat16)
    product = jnp.dot(scaled, weight_matrix, preferred_element_type=jnp.float32)
    return (product * inverse[:, None]).astype(jnp.bfloat16)

def softmax_rows(scores):
    top_score = lax.optimization_barrier(jnp.max(scores, axis=-1, keepdims=True))
    expons = jnp.exp(scores - top_score)
    return (expons / lax.optimization_barrier(jnp.sum(expons, axis=-1, keepdims=True))).astype(jnp.bfloat16)

def spatial_attend(query_rows, key_rows, value_rows, valid_keys):
    scores = jnp.einsum('qhe,khe->hqk', query_rows.astype(jnp.float32), key_rows.astype(jnp.float32))
    scores = scores * HEAD_DIM ** (-0.5)
    scores = jnp.where(valid_keys[None, None, :], scores, -jnp.inf)
    weights = softmax_rows(scores)
    result = jnp.einsum('hqk,khe->qhe', weights.astype(jnp.float32), value_rows.astype(jnp.float32))
    return result.astype(jnp.bfloat16)

def reference(video_tokens, text_tokens, text_length, guide_numer, guide_denom, spatial_gain, spatial_qkv, spatial_out, temporal_gain, temporal_qkv, temporal_out):
    frames_all = video_tokens.shape[1]
    spatial_cols = jnp.transpose(spatial_qkv, (2, 0, 1)).reshape(D, 3 * D)
    temporal_cols = jnp.transpose(temporal_qkv, (2, 0, 1)).reshape(D, 3 * D)
    spatial_right = jnp.transpose(spatial_out)
    temporal_right = jnp.transpose(temporal_out)
    outputs = []
    for branch in range(2):
        video_rows = jnp.swapaxes(video_tokens[branch], 1, 2)
        text_rows = jnp.swapaxes(text_tokens[branch], 1, 2)

        def frame_step(inputs):
            frame_rows, frame_text, live_count = inputs
            mixed = normed_project(frame_rows, spatial_gain, spatial_cols).reshape(POS, 3, HEADS, HEAD_DIM)
            context = normed_project(frame_text, spatial_gain, spatial_cols).reshape(TXT, 3, HEADS, HEAD_DIM)
            key_rows = jnp.concatenate([mixed[:, 1], context[:, 1]], axis=0)
            value_rows = jnp.concatenate([mixed[:, 2], context[:, 2]], axis=0)
            valid_keys = jnp.concatenate([jnp.ones((POS,), dtype=bool), jnp.arange(TXT, dtype=jnp.int32) < live_count])
            attended = spatial_attend(mixed[:, 0], key_rows, value_rows, valid_keys).reshape(POS, D)
            update = jnp.dot(attended, spatial_right, preferred_element_type=jnp.float32)
            return (frame_rows.astype(jnp.float32) + update).astype(jnp.bfloat16)
        after_spatial = lax.map(frame_step, (video_rows, text_rows, text_length[branch]))
        flat_rows = after_spatial.reshape(frames_all * POS, D)
        mixed_time = normed_project(flat_rows, temporal_gain, temporal_cols).reshape(frames_all, POS, 3, HEADS, HEAD_DIM)
        scores = jnp.einsum('fphe,gphe->phfg', mixed_time[:, :, 0].astype(jnp.float32), mixed_time[:, :, 1].astype(jnp.float32))
        weights = softmax_rows(scores * HEAD_DIM ** (-0.5))
        attended_time = jnp.einsum('phfg,gphe->fphe', weights.astype(jnp.float32), mixed_time[:, :, 2].astype(jnp.float32))
        attended_time = attended_time.astype(jnp.bfloat16).reshape(frames_all * POS, D)
        update_time = jnp.dot(attended_time, temporal_right, preferred_element_type=jnp.float32)
        block_out = (flat_rows.astype(jnp.float32) + update_time).astype(jnp.bfloat16)
        outputs.append(block_out.reshape(frames_all, POS, D).astype(jnp.float32))
    ratio = guide_numer.astype(jnp.float32) / guide_denom.astype(jnp.float32)
    cond_out = outputs[0]
    uncond_out = outputs[1]
    guided_rows = (uncond_out + ratio[:, None, None] * (cond_out - uncond_out)).astype(jnp.bfloat16)
    return jnp.swapaxes(guided_rows, 1, 2)
```

```python
import functools

import jax
import jax.numpy as jnp
from jax import lax
from jax.experimental import pallas as pl
from jax.experimental.pallas import tpu as pltpu
from jax.sharding import PartitionSpec as P

D = 1152
HEAD_DIM = 72
epsilon = 1e-06


def shifted(shard, axis, step):
    count = lax.axis_size(axis)
    return lax.ppermute(shard, axis, [(i, (i + step) % count) for i in range(count)])


def gather_features(piece):
    count = lax.axis_size("heads")
    mine = lax.axis_index("heads")
    width = piece.shape[0]
    others = [shifted(piece, "heads", j) for j in range(1, count)]
    if count == 2:
        other = others[0]
        return jnp.where(
            mine == 0,
            jnp.concatenate([piece, other], axis=0),
            jnp.concatenate([other, piece], axis=0),
        )
    full = jnp.zeros((width * count,) + piece.shape[1:], piece.dtype)
    for j, block in enumerate([piece] + others):
        full = lax.dynamic_update_slice_in_dim(full, block, ((mine - j) % count) * width, 0)
    return full


def project(full, gain, weights):
    wide = full.astype(jnp.float32)
    inverse = lax.rsqrt(jnp.mean(wide * wide, axis=0) + epsilon)
    scaled = (wide * gain.astype(jnp.float32)[:, None]).astype(jnp.bfloat16)
    product = jnp.dot(weights, scaled, preferred_element_type=jnp.float32)
    return (product * inverse[None, :]).astype(jnp.bfloat16)


def attend_kernel(positions, length_ref, q_ref, k_ref, v_ref, out_ref):
    scores = lax.dot_general(
        k_ref[0], q_ref[0], (((0,), (0,)), ((), ())), preferred_element_type=jnp.float32
    )
    scores = scores * HEAD_DIM ** (-0.5)
    key_ids = lax.broadcasted_iota(jnp.int32, scores.shape, 0)
    scores = jnp.where(key_ids < positions + length_ref[0], scores, -jnp.inf)
    top = jnp.max(scores, axis=0, keepdims=True)
    expons = jnp.exp(scores - top)
    total = jnp.sum(expons, axis=0, keepdims=True)
    mixed = jnp.dot(v_ref[0], expons.astype(jnp.bfloat16), preferred_element_type=jnp.float32)
    out_ref[0] = (mixed / total).astype(out_ref.dtype)


def attend(length, query, keys, values):
    heads, depth, rows = query.shape
    key_count = keys.shape[2]
    text = key_count
    whole = pl.BlockSpec((1, depth, key_count), lambda h, n: (h, 0, 0))
    part = pl.BlockSpec((1, depth, rows), lambda h, n: (h, 0, 0))
    return lambda positions: pl.pallas_call(
        functools.partial(attend_kernel, positions),
        out_shape=jax.ShapeDtypeStruct(query.shape, jnp.bfloat16),
        grid_spec=pltpu.PrefetchScalarGridSpec(
            num_scalar_prefetch=1, grid=(heads,), in_specs=[part, whole, whole], out_specs=part
        ),
        cost_estimate=pl.CostEstimate(
            flops=16 * heads * rows * text * depth,
            bytes_accessed=2 * heads * depth * (2 * rows + 2 * text),
            transcendentals=heads * rows * text,
        ),
        compiler_params=pltpu.CompilerParams(vmem_limit_bytes=24 * 1024 * 1024),
        name="spatial_attention",
    )(length, query, keys, values)


def shards(
    video_tokens,
    text_tokens,
    text_length,
    guide_numer,
    guide_denom,
    spatial_gain,
    spatial_qkv,
    spatial_out,
    temporal_gain,
    temporal_qkv,
    temporal_out,
):
    frame = video_tokens[0, 0]
    text = text_tokens[0, 0]
    width, positions = frame.shape
    local_heads = width // HEAD_DIM
    steps = lax.axis_size("seq")
    here = lax.axis_index("seq")
    chunk = positions // steps
    branch = lax.axis_index("cfg")
    half = width // 2
    ratio = guide_numer.astype(jnp.float32) / guide_denom.astype(jnp.float32)
    ratios = [ratio] + [shifted(ratio, "seq", k) for k in range(1, steps)]

    spatial_weights = spatial_qkv.reshape(3 * width, D)
    temporal_weights = temporal_qkv.reshape(3 * width, D)
    context = project(gather_features(text), spatial_gain, spatial_weights[width:])
    context = context.reshape(2, local_heads, HEAD_DIM, -1)
    pieces = 2
    span = positions // pieces
    parts = []
    for i in range(pieces):
        full = gather_features(frame[:, i * span : (i + 1) * span])
        part = project(full, spatial_gain, spatial_weights)
        parts.append(part.reshape(3, local_heads, HEAD_DIM, span))
    keys = jnp.concatenate([part[1] for part in parts] + [context[0]], axis=2)
    values = jnp.concatenate([part[2] for part in parts] + [context[1]], axis=2)
    queries = jnp.concatenate([part[0] for part in parts], axis=2)

    order = list(range(1, steps)) + [0]
    rows = {}
    for k in order:
        start = ((here + k) % steps) * chunk
        query = lax.dynamic_slice_in_dim(queries, start, chunk, 2)
        attended = attend(text_length[0], query, keys, values)(positions)
        full = gather_features(attended.reshape(width, chunk))
        update = jnp.dot(spatial_out, full, preferred_element_type=jnp.float32)
        base = lax.dynamic_slice_in_dim(frame, start, chunk, 1).astype(jnp.float32)
        state = (base + update).astype(jnp.bfloat16)
        rows[k] = state if k == 0 else shifted(state, "seq", k)

    mixed = {}
    for k in order:
        part = project(gather_features(rows[k]), temporal_gain, temporal_weights)
        mixed[k] = part.reshape(3, local_heads, HEAD_DIM, chunk)

    backs = {}
    for k in order:
        query = mixed[k][0].astype(jnp.float32)
        scores = [
            jnp.sum(query * mixed[g][1].astype(jnp.float32), axis=1) * HEAD_DIM ** (-0.5)
            for g in range(steps)
        ]
        top = functools.reduce(jnp.maximum, scores)
        expons = [jnp.exp(score - top) for score in scores]
        total = functools.reduce(jnp.add, expons)
        acc = 0.0
        for g in range(steps):
            weight = (expons[g] / total).astype(jnp.bfloat16).astype(jnp.float32)
            acc = acc + weight[:, None, :] * mixed[g][2].astype(jnp.float32)
        attended = acc.astype(jnp.bfloat16).reshape(width, chunk)
        update = jnp.dot(
            temporal_out, gather_features(attended), preferred_element_type=jnp.float32
        )
        block = (rows[k].astype(jnp.float32) + update).astype(jnp.bfloat16)
        keep = jnp.where(branch == 0, block[:half], block[half:])
        give = jnp.where(branch == 0, block[half:], block[:half])
        got = shifted(give, "cfg", 1)
        cond = jnp.where(branch == 0, keep, got).astype(jnp.float32)
        uncond = jnp.where(branch == 0, got, keep).astype(jnp.float32)
        guided = (uncond + ratios[k] * (cond - uncond)).astype(jnp.bfloat16)
        backs[k] = guided if k == 0 else shifted(guided, "seq", -k)

    result = jnp.zeros((half, positions), jnp.bfloat16)
    for k in order:
        start = ((here + k) % steps) * chunk
        result = lax.dynamic_update_slice_in_dim(result, backs[k], start, 1)
    return result[None]


def from_partner(shard, axis, stride):
    return lax.ppermute(shard, axis, [(i, i ^ 1 << stride) for i in range(lax.axis_size(axis))])


def softmax_along(scores, axis):
    top_score = jnp.max(scores, axis=axis, keepdims=True)
    expons = jnp.exp(scores - top_score)
    return (expons / jnp.sum(expons, axis=axis, keepdims=True)).astype(jnp.bfloat16)


def project_piece(piece, gain_vector, weights, parts):
    gain_piece = gain_vector.astype(jnp.float32)
    weight_piece = weights[parts]
    piece_wide = piece.astype(jnp.float32)
    scaled = (piece_wide * gain_piece[None, :, None]).astype(jnp.bfloat16)
    product = jnp.einsum("kod,fdp->fkop", weight_piece, scaled, preferred_element_type=jnp.float32)
    return (product, jnp.sum(piece_wide * piece_wide, axis=1))


def add_mixed(piece, matrix):
    return jnp.einsum("oc,fcp->fop", matrix, piece, preferred_element_type=jnp.float32)


def shards_many(
    video_tokens,
    text_tokens,
    text_length,
    guide_numer,
    guide_denom,
    spatial_gain,
    spatial_qkv,
    spatial_out,
    temporal_gain,
    temporal_qkv,
    temporal_out,
):
    frame_count = video_tokens.shape[1]
    width = video_tokens.shape[2]
    positions = video_tokens.shape[3]
    text_count = text_tokens.shape[3]
    local_heads = width // HEAD_DIM
    frame_tokens = video_tokens[0]
    frame_text = text_tokens[0]
    video_piece = lax.all_gather(frame_tokens, "heads", axis=1, tiled=True)
    text_piece = lax.all_gather(frame_text, "heads", axis=1, tiled=True)
    video_add, video_sq = project_piece(video_piece, spatial_gain, spatial_qkv, slice(0, 3))
    text_add, text_sq = project_piece(text_piece, spatial_gain, spatial_qkv, slice(1, 3))
    mixed = (video_add * lax.rsqrt(video_sq / D + epsilon)[:, None, None, :]).astype(jnp.bfloat16)
    mixed = mixed.reshape(frame_count, 3, local_heads, HEAD_DIM, positions)
    context = (text_add * lax.rsqrt(text_sq / D + epsilon)[:, None, None, :]).astype(jnp.bfloat16)
    context = context.reshape(frame_count, 2, local_heads, HEAD_DIM, text_count)
    key_rows = jnp.concatenate([mixed[:, 1], context[:, 0]], axis=3)
    value_rows = jnp.concatenate([mixed[:, 2], context[:, 1]], axis=3)
    query_all = mixed[:, 0]
    text_valid = jnp.arange(text_count, dtype=jnp.int32)[None, :] < text_length[0][:, None]
    valid_keys = jnp.concatenate(
        [jnp.ones((frame_count, positions), dtype=bool), text_valid], axis=1
    )
    block_rows = min(512, positions)
    block_count = positions // block_rows
    frame_ids = jnp.repeat(jnp.arange(frame_count, dtype=jnp.int32), block_count)
    block_ids = jnp.tile(jnp.arange(block_count, dtype=jnp.int32), frame_count)

    def block_step(inputs):
        frame_id, block_id = inputs
        query_rows = lax.dynamic_slice_in_dim(
            query_all[frame_id], block_id * block_rows, block_rows, 2
        )
        scores = jnp.einsum(
            "hep,hek->hpk", query_rows, key_rows[frame_id], preferred_element_type=jnp.float32
        )
        scores = scores * HEAD_DIM ** (-0.5)
        scores = jnp.where(valid_keys[frame_id][None, None, :], scores, -jnp.inf)
        weights = softmax_along(scores, 2)
        result = jnp.einsum(
            "hpk,hek->hep", weights, value_rows[frame_id], preferred_element_type=jnp.float32
        )
        return result.astype(jnp.bfloat16)

    attended = lax.map(block_step, (frame_ids, block_ids))
    attended = attended.reshape(frame_count, block_count, local_heads, HEAD_DIM, block_rows)
    attended = jnp.transpose(attended, (0, 2, 3, 1, 4)).reshape(frame_count, width, positions)
    update = add_mixed(lax.all_gather(attended, "heads", axis=1, tiled=True), spatial_out)
    after_spatial = (frame_tokens.astype(jnp.float32) + update).astype(jnp.bfloat16)
    own_rows = lax.all_to_all(after_spatial, "seq", split_axis=2, concat_axis=0, tiled=True)
    frames_all = own_rows.shape[0]
    columns = own_rows.shape[2]
    piece_add, piece_sq = project_piece(
        lax.all_gather(own_rows, "heads", axis=1, tiled=True),
        temporal_gain,
        temporal_qkv,
        slice(0, 3),
    )
    mixed_time = (piece_add * lax.rsqrt(piece_sq / D + epsilon)[:, None, None, :]).astype(
        jnp.bfloat16
    )
    mixed_time = mixed_time.reshape(frames_all, 3, local_heads, HEAD_DIM, columns)
    time_scores = jnp.einsum(
        "fhep,ghep->hfgp", mixed_time[:, 0], mixed_time[:, 1], preferred_element_type=jnp.float32
    )
    time_weights = softmax_along(time_scores * HEAD_DIM ** (-0.5), 2)
    attended_time = jnp.einsum(
        "hfgp,ghep->fhep", time_weights, mixed_time[:, 2], preferred_element_type=jnp.float32
    )
    attended_time = attended_time.astype(jnp.bfloat16).reshape(frames_all, width, columns)
    update_time = add_mixed(
        lax.all_gather(attended_time, "heads", axis=1, tiled=True), temporal_out
    )
    block_out = (own_rows.astype(jnp.float32) + update_time).astype(jnp.bfloat16)
    returned = lax.all_to_all(block_out, "seq", split_axis=0, concat_axis=2, tiled=True)
    half_width = width // 2
    partner = from_partner(returned, "cfg", 0)
    branch_index = lax.axis_index("cfg")
    cond_full = jnp.where(branch_index == 0, returned, partner)
    uncond_full = jnp.where(branch_index == 0, partner, returned)
    cond_part = lax.dynamic_slice_in_dim(cond_full, branch_index * half_width, half_width, 1)
    uncond_part = lax.dynamic_slice_in_dim(uncond_full, branch_index * half_width, half_width, 1)
    ratio = guide_numer.astype(jnp.float32) / guide_denom.astype(jnp.float32)
    cond_wide = cond_part.astype(jnp.float32)
    uncond_wide = uncond_part.astype(jnp.float32)
    return (uncond_wide + ratio[:, None, None] * (cond_wide - uncond_wide)).astype(jnp.bfloat16)


def solution(mesh):
    return jax.shard_map(
        shards if mesh.shape["seq"] * mesh.shape["heads"] <= 8 else shards_many,
        mesh=mesh,
        in_specs=(
            P("cfg", ("groups", "seq"), "heads", None),
            P("cfg", ("groups", "seq"), "heads", None),
            P("cfg", ("groups", "seq")),
            P(("groups", "seq")),
            P(("groups", "seq")),
            P(),
            P(None, "heads", None),
            P("heads", None),
            P(),
            P(None, "heads", None),
            P("heads", None),
        ),
        out_specs=P(("groups", "seq"), ("heads", "cfg"), None),
        check_vma=False,
    )
```
